32 devices in a mesh: groups: 2 (over x), tok: 16 (over z, y, core).
Axes of the slice: x: 2, y: 2, z: 4, core: 2. Of those that a mesh axis runs over, the one named last changes fastest.
Arguments:
- activations: bfloat16 [32, 128, 768], P(('groups', 'tok')), parts along dimension 0, may hold values from -32 to 32
- pair_repr: bfloat16 [256, 128, 128], P('groups', 'tok'), parts along dimension 0, may hold values from -6 to 6
- pair_gain: float32 [128], replicated, may hold values from 0.5 to 1.5
- bias_weight: float32 [128, 16], replicated, may hold values from -0.5 to 0.5
- proj_weight: bfloat16 [768, 3072], replicated, may hold values from -0.21875 to 0.21875
- query_bias: float32 [768], replicated, may hold values from -5 to 5
- out_weight: bfloat16 [768, 768], replicated, may hold values from -0.21875 to 0.21875
- token_mask: int32 [256], P('groups'), parts along dimension 0, may hold values 0 or 1
- out_cotangent: bfloat16 [32, 128, 768], P(('groups', 'tok')), parts along dimension 0, may hold values from -6 to 6
Outputs:
- grad_activations: bfloat16 [32, 128, 768], P(('groups', 'tok')), parts along dimension 0
- grad_pair: bfloat16 [256, 128, 128], P('groups', 'tok'), parts along dimension 0
- grad_proj: float32 [1536, 3072], P(('groups', 'tok')), parts along dimension 0
- grad_out_weight: float32 [1536, 768], P(('groups', 'tok')), parts along dimension 0
- grad_query_bias: float32 [1536], P('groups'), parts along dimension 0
- grad_bias_weight: float32 [256, 16], P('groups'), parts along dimension 0
- grad_pair_gain: float32 [256], P('groups'), parts along dimension 0
The draws below stay inside these ranges and needn't reach their ends.
There are 2 independent parts, one for each index of `groups`. The reference program is written for one: setup_inputs(seed, part) draws one part's arguments, and reference() takes and returns one part's arrays. A program takes and returns all parts, laid end to end along the dimension named above; an argument that names none is the same for every part. Nothing has to cross between parts.
All inputs are finite; a program needn't handle non-finite values.
Results may differ from the reference program's by a relative error of at most 0.015.
The reference program's roundings to bfloat16 on the way count: a program that leaves them out, or rounds other values in their place, can miss the bound.
Values may be sent and summed in bfloat16 or wider, within the bound.
A program may use at most 128 MiB of HBM per device.

```python
import jax
import jax.numpy as jnp
from jax import lax

D = 768
HEADS = 16
HD = 48
CZ = 128
NTOK = 128
SAMPLES = 16


def draw_activations(key, part):
    values = jax.random.truncated_normal(key, -4.0, 4.0, (SAMPLES, NTOK, D), jnp.float32)
    return values.astype(jnp.bfloat16)


def set_ends(result, stream_key, least, top_value):
    spot = [jax.random.randint(jax.random.fold_in(stream_key, axis), (), 0, length) for axis, length in enumerate(result.shape)]
    main_axis = result.shape.index(max(result.shape))
    next_to = spot[:main_axis] + [(spot[main_axis] + 1) % result.shape[main_axis]] + spot[main_axis + 1:]
    return result.at[tuple(spot)].set(least).at[tuple(next_to)].set(top_value)


def with_spikes(drawn, rng, source, target, blocks, factor):
    def block_of(axis_at):
        return (jnp.arange(drawn.shape[axis_at]) // (drawn.shape[axis_at] // blocks)).reshape((-1,) + (1,) * (drawn.ndim - 1 - axis_at))

    one_side = jax.random.permutation(rng, blocks)[block_of(target)]
    other_side = (block_of(target) + blocks // 2) % blocks
    return jnp.where((block_of(source) == one_side) | (block_of(source) == other_side), factor * drawn, drawn)


def shard_levels(rng, shape, shards, smallest, top_value):
    loudness = 1.0
    for dim, shards_of in shards:
        draws = jax.random.uniform(jax.random.fold_in(jax.random.fold_in(rng, 6), dim), (shards_of,), jnp.float32, smallest / len(shards), top_value / len(shards))
        loudness = loudness * jnp.repeat(jnp.exp(draws), shape[dim] // shards_of).reshape((-1,) + (1,) * (len(shape) - 1 - dim))
    return loudness


def scatter_about(rng, dims, scale, reach, shards=(), dtype=jnp.bfloat16):
    values = jax.random.normal(rng, dims, jnp.float32) * scale
    if len(shards) > 0:
        values = shard_levels(rng, dims, shards, -0.22, 0.18) * values
    return jnp.clip(values, min=-reach, max=reach).astype(dtype)


def gaussian_with(key, dims, scale, reach, cuts, heavy, kind=jnp.bfloat16):
    drawn = scale * jax.random.normal(key, dims, jnp.float32)
    if cuts:
        drawn = drawn * shard_levels(key, dims, cuts, -0.22, 0.18)
    return jnp.clip(with_spikes(drawn, jax.random.fold_in(key, 3), *heavy), -reach, reach).astype(kind)


def setup_inputs(seed: int = 0, part: int = 0) -> dict:
    seeds = jax.random.split(jax.random.key(seed), 10)
    own_keys = jax.random.split(jax.random.fold_in(seeds[9], part), 10)
    return {
        "activations": draw_activations(jax.random.fold_in(jax.random.fold_in(seeds[9], part), 71), part),
        "pair_repr": scatter_about(own_keys[1], (NTOK, NTOK, CZ), 1.0, 6.0, ((1, 16),)),
        "pair_gain": jnp.clip(1.0 + 0.1 * jax.random.normal(seeds[2], (CZ,), jnp.float32), 0.5, 1.5),
        "bias_weight": scatter_about(seeds[3], (CZ, HEADS), CZ ** -0.5, 0.5, (), jnp.float32),
        "proj_weight": scatter_about(seeds[4], (D, 4 * D), D ** -0.5, 0.21875),
        "query_bias": scatter_about(seeds[5], (D,), 1.0, 5.0, (), jnp.float32),
        "out_weight": scatter_about(seeds[6], (D, D), D ** -0.5, 0.21875),
        "token_mask": set_ends((jax.random.randint(own_keys[7], (NTOK,), 0, 8) < 7).astype(jnp.int32), jax.random.fold_in(own_keys[7], 1), 0, 1),
        "out_cotangent": gaussian_with(own_keys[8], (SAMPLES, NTOK, D), 1.0, 6.0, ((0, 16),), (0, 2, 16, 2.0)),
    }


EPSILON = 1e-05
MASK_PENALTY = 10000.0

def reference(activations, pair_repr, pair_gain, bias_weight, proj_weight, query_bias, out_weight, token_mask, out_cotangent):
    feature = activations.shape[2]
    all_tokens = activations.shape[1]
    softmax_scale = HD ** (-0.5)
    act_rows = activations.reshape(SAMPLES * all_tokens, feature)
    cot_rows = out_cotangent.reshape(SAMPLES * all_tokens, feature)
    proj = jnp.dot(act_rows, proj_weight, preferred_element_type=jnp.float32)
    shift = jnp.concatenate([query_bias, jnp.zeros((2 * feature,), jnp.float32)])
    qkv_rows = (proj[:, :3 * feature] + shift[None, :]).astype(jnp.bfloat16)
    gate = jax.nn.sigmoid(proj[:, 3 * feature:]).astype(jnp.bfloat16)
    pair_f = pair_repr.astype(jnp.float32)
    mean_z = lax.optimization_barrier(jnp.mean(pair_f, axis=-1, keepdims=True))
    centred = pair_f - mean_z
    rstd = lax.rsqrt(lax.optimization_barrier(jnp.mean(centred * centred, axis=-1, keepdims=True)) + EPSILON)
    normed = centred * rstd
    scaled = normed * pair_gain
    pair_bias = jnp.einsum('ijc,ch->hij', scaled, bias_weight, precision=lax.Precision.HIGHEST).astype(jnp.bfloat16)
    bias_full = pair_bias.astype(jnp.float32)
    key_bias = (token_mask.astype(jnp.float32) - 1.0) * MASK_PENALTY
    grad_gated = jnp.dot(cot_rows, out_weight.T, preferred_element_type=jnp.float32).astype(jnp.bfloat16)
    qkv_s = qkv_rows.reshape(SAMPLES, all_tokens, 3, HEADS, HD)
    gate_s = gate.reshape(SAMPLES, all_tokens, feature)
    grad_s_in = grad_gated.reshape(SAMPLES, all_tokens, feature)

    def per_sample(total, pieces):
        qkv, gate_one, grad_one = pieces
        query = qkv[:, 0].transpose(1, 0, 2).astype(jnp.float32)
        keys = qkv[:, 1].transpose(1, 0, 2).astype(jnp.float32)
        values = qkv[:, 2].transpose(1, 0, 2).astype(jnp.float32)
        scores = jnp.einsum('hid,hjd->hij', query, keys) * softmax_scale + bias_full + key_bias[None, None, :]
        peak = lax.optimization_barrier(jnp.max(scores, axis=-1, keepdims=True))
        expo = jnp.exp(scores - peak)
        probs = expo / lax.optimization_barrier(jnp.sum(expo, axis=-1, keepdims=True))
        probs_b = probs.astype(jnp.bfloat16).astype(jnp.float32)
        attended = jnp.einsum('hij,hjd->hid', probs_b, values).astype(jnp.bfloat16)
        attended = attended.transpose(1, 0, 2).reshape(all_tokens, feature).astype(jnp.float32)
        gate32 = gate_one.astype(jnp.float32)
        grad32 = grad_one.astype(jnp.float32)
        gated = (gate32 * attended).astype(jnp.bfloat16)
        grad_att = (grad32 * gate32).astype(jnp.bfloat16)
        grad_logit = (grad32 * attended * gate32 * (1.0 - gate32)).astype(jnp.bfloat16)
        grad_heads = grad_att.reshape(all_tokens, HEADS, HD).transpose(1, 0, 2).astype(jnp.float32)
        grad_probs = jnp.einsum('hid,hjd->hij', grad_heads, values)
        grad_scores = probs * (grad_probs - lax.optimization_barrier(jnp.sum(probs * grad_probs, axis=-1, keepdims=True)))
        scores_b = grad_scores.astype(jnp.bfloat16).astype(jnp.float32)
        grad_query = jnp.einsum('hij,hjd->hid', scores_b, keys) * softmax_scale
        grad_value = jnp.einsum('hij,hid->hjd', probs_b, grad_heads)
        grad_key = jnp.einsum('hij,hid->hjd', scores_b, query) * softmax_scale
        stacked = jnp.stack([grad_query, grad_key, grad_value], axis=0).astype(jnp.bfloat16)
        stacked = stacked.transpose(2, 0, 1, 3).reshape(all_tokens, 3 * feature)
        rows_out = jnp.concatenate([stacked, grad_logit], axis=1)
        return (total + grad_scores, (rows_out, gated))
    start_total = jnp.zeros((HEADS, all_tokens, all_tokens), jnp.float32)
    grad_bias, outs = lax.scan(per_sample, start_total, (qkv_s, gate_s, grad_s_in))
    grad_rows = outs[0].reshape(SAMPLES * all_tokens, 4 * feature)
    gated_rows = outs[1].reshape(SAMPLES * all_tokens, feature)
    grad_proj = jnp.dot(act_rows.T, grad_rows, preferred_element_type=jnp.float32)
    grad_out_weight = jnp.dot(gated_rows.T, cot_rows, preferred_element_type=jnp.float32)
    grad_query_bias = lax.optimization_barrier(jnp.sum(grad_rows[:, :feature].astype(jnp.float32), axis=0))
    grad_activations = jnp.dot(grad_rows, proj_weight.T, preferred_element_type=jnp.float32).astype(jnp.bfloat16)
    grad_zg = jnp.einsum('hij,ch->ijc', grad_bias, bias_weight, precision=lax.Precision.HIGHEST)
    grad_bias_weight = jnp.einsum('ijc,hij->ch', scaled, grad_bias, precision=lax.Precision.HIGHEST)
    grad_pair_gain = lax.optimization_barrier(jnp.sum(normed * grad_zg, axis=(0, 1)))
    grad_norm = grad_zg * pair_gain
    grad_pair = (grad_norm - lax.optimization_barrier(jnp.mean(grad_norm, axis=-1, keepdims=True)) - normed * lax.optimization_barrier(jnp.mean(grad_norm * normed, axis=-1, keepdims=True))) * rstd
    return (grad_activations.reshape(SAMPLES, all_tokens, feature), grad_pair.astype(jnp.bfloat16), grad_proj, grad_out_weight, grad_query_bias, grad_bias_weight, grad_pair_gain)
```

```python
import jax
import jax.numpy as jnp
from jax import lax
from jax.sharding import PartitionSpec as P

HEADS = 16
HD = 48
EPSILON = 1e-05
MASK_PENALTY = 10000.0
F32 = jnp.float32
BF16 = jnp.bfloat16


def attention(query, keys, values, gate, grad_gated, bias_t, key_bias):
    scale = HD ** (-0.5)
    scores = jnp.einsum("hdj,hdi->hji", keys, query, preferred_element_type=F32) * scale
    scores = scores + bias_t.transpose(1, 0, 2).astype(F32) + key_bias[None, :, None]
    peak = jnp.max(scores, axis=1, keepdims=True)
    expo = jnp.exp(scores - peak)
    probs = expo / jnp.sum(expo, axis=1, keepdims=True)
    probs_b = probs.astype(BF16)
    attended = jnp.einsum("hdj,hji->hdi", values, probs_b, preferred_element_type=F32).astype(BF16)
    gate32 = gate.astype(F32)
    grad32 = grad_gated.astype(F32)
    att32 = attended.astype(F32)
    gated = (gate32 * att32).astype(BF16)
    grad_att = (grad32 * gate32).astype(BF16)
    grad_logit = (grad32 * att32 * gate32 * (1.0 - gate32)).astype(BF16)
    grad_probs = jnp.einsum("hdj,hdi->hji", values, grad_att, preferred_element_type=F32)
    grad_scores = probs * (grad_probs - jnp.sum(probs * grad_probs, axis=1, keepdims=True))
    scores_b = grad_scores.astype(BF16)
    grad_query = (jnp.einsum("hdj,hji->hdi", keys, scores_b, preferred_element_type=F32) * scale).astype(BF16)
    grad_key = (jnp.einsum("hdi,hji->hdj", query, scores_b, preferred_element_type=F32) * scale).astype(BF16)
    grad_value = jnp.einsum("hdi,hji->hdj", grad_att, probs_b, preferred_element_type=F32).astype(BF16)
    return jnp.stack([grad_query, grad_key, grad_value, grad_logit]), gated, grad_scores


def on_device(activations, pair_repr, pair_gain, bias_weight, proj_weight, query_bias, out_weight, token_mask, out_cotangent):
    samples, tokens, feature = activations.shape
    tok = lax.axis_size("tok")
    cols = pair_repr.shape[1]
    act = activations.reshape(samples * tokens, feature)
    cot = out_cotangent.reshape(samples * tokens, feature)
    pair_f = pair_repr.astype(F32)
    centred = pair_f - jnp.mean(pair_f, axis=-1, keepdims=True)
    rstd = lax.rsqrt(jnp.mean(centred * centred, axis=-1, keepdims=True) + EPSILON)
    normed = centred * rstd
    scaled = normed * pair_gain
    bias_cols = jnp.einsum("ijc,ch->jhi", scaled, bias_weight, precision=lax.Precision.HIGHEST).astype(BF16)
    bias_t = lax.all_gather(bias_cols, "tok", axis=0, tiled=True)
    proj = jnp.einsum("tf,fn->nt", act, proj_weight, preferred_element_type=F32)
    proj = proj.reshape(4, feature, samples * tokens)
    query = (proj[0] + query_bias[:, None]).astype(BF16)
    keys = proj[1].astype(BF16)
    values = proj[2].astype(BF16)
    gate = jax.nn.sigmoid(proj[3]).astype(BF16)
    grad_gated = jnp.einsum("tn,mn->mt", cot, out_weight, preferred_element_type=F32).astype(BF16)
    key_bias = (token_mask.astype(F32) - 1.0) * MASK_PENALTY

    def heads_of(x):
        return x.reshape(HEADS, HD, samples, tokens).transpose(2, 0, 1, 3)

    grads, gated, grad_scores = jax.vmap(attention, in_axes=(0, 0, 0, 0, 0, None, None))(
        heads_of(query), heads_of(keys), heads_of(values), heads_of(gate), heads_of(grad_gated), bias_t, key_bias
    )
    grad_rows = grads.transpose(1, 2, 3, 0, 4).reshape(4 * feature, samples * tokens)
    gated_t = gated.transpose(1, 2, 0, 3).reshape(feature, samples * tokens)
    first = jnp.einsum("tr,nt->rn", act, grad_rows, preferred_element_type=F32)
    second = jnp.einsum("rt,tn->rn", gated_t, cot, preferred_element_type=F32)
    terms = jnp.concatenate([first.astype(BF16), second.astype(BF16)], axis=1)
    score_sum = jnp.sum(grad_scores, axis=0).astype(BF16)
    outgoing = score_sum.reshape(HEADS, tok, cols, tokens).transpose(1, 2, 0, 3)
    received = lax.all_to_all(outgoing, "tok", split_axis=0, concat_axis=0, tiled=True)
    grad_bias = jnp.sum(received.astype(F32), axis=0)
    grad_activations = jnp.einsum("nt,fn->tf", grad_rows, proj_weight, preferred_element_type=F32).astype(BF16)
    grad_zg = jnp.einsum("jhi,ch->ijc", grad_bias, bias_weight, precision=lax.Precision.HIGHEST)
    weight_part = jnp.einsum("ijc,jhi->ch", scaled, grad_bias, precision=lax.Precision.HIGHEST)
    gain_part = jnp.sum(normed * grad_zg, axis=(0, 1))
    query_part = jnp.sum(grad_rows[:feature].astype(F32), axis=1)
    small = jnp.concatenate([query_part, weight_part.reshape(-1), gain_part])
    small = jnp.sum(lax.all_gather(small, "tok", axis=0), axis=0)
    terms, small = lax.optimization_barrier((terms, small))
    weight_grads = lax.psum_scatter(terms, "tok", scatter_dimension=0, tiled=True).astype(F32)
    grad_norm = grad_zg * pair_gain
    grad_pair = (
        grad_norm
        - jnp.mean(grad_norm, axis=-1, keepdims=True)
        - normed * jnp.mean(grad_norm * normed, axis=-1, keepdims=True)
    ) * rstd
    split = feature + weight_part.size
    return (
        grad_activations.reshape(samples, tokens, feature),
        grad_pair.astype(BF16),
        weight_grads[:, : 4 * feature],
        weight_grads[:, 4 * feature :],
        small[:feature],
        small[feature:split].reshape(weight_part.shape),
        small[split:],
    )


def solution(mesh):
    in_specs = (
        P(("groups", "tok"), None, None),
        P("groups", "tok", None),
        P(),
        P(),
        P(),
        P(),
        P(),
        P("groups"),
        P(("groups", "tok"), None, None),
    )
    out_specs = (
        P(("groups", "tok"), None, None),
        P("groups", "tok", None),
        P(("groups", "tok"), None),
        P(("groups", "tok"), None),
        P("groups"),
        P("groups", None),
        P("groups"),
    )
    return jax.shard_map(on_device, mesh=mesh, in_specs=in_specs, out_specs=out_specs, check_vma=False)
```

```python
import functools

import jax
import jax.numpy as jnp
from jax import lax
from jax.experimental import pallas as pl
from jax.experimental.pallas import tpu as pltpu
from jax.sharding import PartitionSpec as P

HEADS = 16
HD = 48
EPSILON = 1e-05
MASK_PENALTY = 10000.0
F32 = jnp.float32
BF16 = jnp.bfloat16
INNER = 4


def exchange_kernel(kinds, tok, *refs):
    count = len(kinds)
    ins, outs = refs[:count], refs[count : 2 * count]
    sends, recvs, local_sem = refs[2 * count : 3 * count], refs[3 * count : 4 * count], refs[4 * count]
    me = lax.axis_index("tok")
    group = me // INNER
    place = me % INNER
    across = place + 1 - 2 * (place % 2)
    beside = place + 2 - 4 * (place // 2)
    barrier = pltpu.get_barrier_semaphore()
    for step in range(1, tok):
        pl.semaphore_signal(barrier, inc=1, device_id={"tok": (me + step) % tok})
    pl.semaphore_wait(barrier, tok - 1)

    def send(k, slot, src, dst, peer):
        copy = pltpu.make_async_remote_copy(
            src_ref=src,
            dst_ref=dst,
            send_sem=sends[k].at[slot],
            recv_sem=recvs[k].at[slot],
            device_id={"tok": peer},
        )
        copy.start()
        return copy

    pending, relays, local = [], [], []
    for k, kind in enumerate(kinds):
        x, out = ins[k], outs[k]
        if kind == "near":
            first = send(k, 0, x, out.at[place], group * INNER + beside)
            pending.append(send(k, 1, x, out.at[place], group * INNER + across))
            relays.append((k, first, out.at[beside]))
        elif kind in ("all", "each"):
            for step in range(1, tok):
                peer = (me + step) % tok
                pending.append(send(k, step - 1, x if kind == "all" else x.at[peer], out.at[me], peer))
        elif kind == "near_each":
            for step in range(1, INNER):
                other = (place + step) % INNER
                pending.append(send(k, step - 1, x.at[other], out.at[place], group * INNER + other))
        else:
            for step in range(1, tok // INNER):
                other = (group + step) % (tok // INNER)
                pending.append(send(k, step - 1, x.at[other], out.at[group], other * INNER + place))
    for k, kind in enumerate(kinds):
        mine = {"all": me, "each": me, "near": place, "near_each": place, "far_each": group}[kind]
        own = ins[k] if kind in ("all", "near") else ins[k].at[mine]
        copy = pltpu.make_async_copy(own, outs[k].at[mine], local_sem.at[k])
        copy.start()
        local.append(copy)
    for k, first, block in relays:
        first.wait()
        pending.append(send(k, 2, block, block, group * INNER + across))
    for copy in local + pending:
        copy.wait()


def exchange(arrays, kinds, tok, collective_id):
    sizes = {"all": tok, "each": tok, "near": INNER, "near_each": INNER, "far_each": tok // INNER}
    shapes = []
    for x, kind in zip(arrays, kinds):
        block = x.shape if kind in ("all", "near") else x.shape[1:]
        shapes.append(jax.ShapeDtypeStruct((sizes[kind],) + block, x.dtype))
    sems = [pltpu.SemaphoreType.DMA((max(3, sizes[kind] - 1),)) for kind in kinds]
    return pl.pallas_call(
        functools.partial(exchange_kernel, kinds, tok),
        out_shape=shapes,
        in_specs=[pl.BlockSpec(memory_space=pltpu.VMEM)] * len(kinds),
        out_specs=[pl.BlockSpec(memory_space=pltpu.VMEM)] * len(kinds),
        scratch_shapes=sems + sems + [pltpu.SemaphoreType.DMA((len(kinds),))],
        compiler_params=pltpu.CompilerParams(
            collective_id=collective_id, has_side_effects=True, vmem_limit_bytes=40 * 2**20
        ),
        name=f"exchange_{collective_id}",
    )(*arrays)


def attention(query, keys, values, gate, grad_gated, bias_t, key_bias):
    scale = HD ** (-0.5)
    scores = jnp.einsum("hdj,hdi->hji", keys, query, preferred_element_type=F32) * scale
    scores = scores + bias_t.transpose(1, 0, 2).astype(F32) + key_bias[None, :, None]
    peak = jnp.max(scores, axis=1, keepdims=True)
    expo = jnp.exp(scores - peak)
    probs = expo / jnp.sum(expo, axis=1, keepdims=True)
    probs_b = probs.astype(BF16)
    attended = jnp.einsum("hdj,hji->hdi", values, probs_b, preferred_element_type=F32).astype(BF16)
    gate32 = gate.astype(F32)
    grad32 = grad_gated.astype(F32)
    att32 = attended.astype(F32)
    gated = (gate32 * att32).astype(BF16)
    grad_att = (grad32 * gate32).astype(BF16)
    grad_logit = (grad32 * att32 * gate32 * (1.0 - gate32)).astype(BF16)
    grad_probs = jnp.einsum("hdj,hdi->hji", values, grad_att, preferred_element_type=F32)
    grad_scores = probs * (grad_probs - jnp.sum(probs * grad_probs, axis=1, keepdims=True))
    scores_b = grad_scores.astype(BF16)
    grad_query = (jnp.einsum("hdj,hji->hdi", keys, scores_b, preferred_element_type=F32) * scale).astype(BF16)
    grad_key = (jnp.einsum("hdi,hji->hdj", query, scores_b, preferred_element_type=F32) * scale).astype(BF16)
    grad_value = jnp.einsum("hdi,hji->hdj", grad_att, probs_b, preferred_element_type=F32).astype(BF16)
    return jnp.stack([grad_query, grad_key, grad_value, grad_logit]), gated, grad_scores


def on_device(activations, pair_repr, pair_gain, bias_weight, proj_weight, query_bias, out_weight, token_mask, out_cotangent):
    samples, tokens, feature = activations.shape
    tok = lax.axis_size("tok")
    cols = pair_repr.shape[1]
    act = activations.reshape(samples * tokens, feature)
    cot = out_cotangent.reshape(samples * tokens, feature)
    pair_f = pair_repr.astype(F32)
    centred = pair_f - jnp.mean(pair_f, axis=-1, keepdims=True)
    rstd = lax.rsqrt(jnp.mean(centred * centred, axis=-1, keepdims=True) + EPSILON)
    normed = centred * rstd
    scaled = normed * pair_gain
    bias_cols = jnp.einsum("ijc,ch->jhi", scaled, bias_weight, precision=lax.Precision.HIGHEST).astype(BF16)
    outer = tok // INNER
    shard = feature // tok

    def near_blocks(x):
        blocks = x.reshape(outer, INNER, shard, samples * tokens).transpose(1, 0, 2, 3)
        return blocks.reshape(INNER, outer * shard, samples * tokens)

    bias_t, cot_near, act_near = exchange(
        (bias_cols, cot, near_blocks(act.T)), ("all", "near", "near_each"), tok, 0
    )
    bias_t = bias_t.reshape((tok * cols,) + bias_cols.shape[1:])
    proj = jnp.einsum("tf,fn->nt", act, proj_weight, preferred_element_type=F32)
    proj = proj.reshape(4, feature, samples * tokens)
    query = (proj[0] + query_bias[:, None]).astype(BF16)
    keys = proj[1].astype(BF16)
    values = proj[2].astype(BF16)
    gate = jax.nn.sigmoid(proj[3]).astype(BF16)
    grad_gated = jnp.einsum("tn,mn->mt", cot, out_weight, preferred_element_type=F32).astype(BF16)
    key_bias = (token_mask.astype(F32) - 1.0) * MASK_PENALTY

    def heads_of(x):
        return x.reshape(HEADS, HD, samples, tokens).transpose(2, 0, 1, 3)

    grads, gated, grad_scores = jax.vmap(attention, in_axes=(0, 0, 0, 0, 0, None, None))(
        heads_of(query), heads_of(keys), heads_of(values), heads_of(gate), heads_of(grad_gated), bias_t, key_bias
    )
    grad_rows = grads.transpose(1, 2, 3, 0, 4).reshape(4 * feature, samples * tokens)
    gated_t = gated.transpose(1, 2, 0, 3).reshape(feature, samples * tokens)
    score_sum = jnp.sum(grad_scores, axis=0).astype(BF16)
    outgoing = score_sum.reshape(HEADS, tok, cols, tokens).transpose(1, 2, 0, 3)
    received, rows_near, gated_near = exchange(
        (outgoing, grad_rows, near_blocks(gated_t)), ("each", "near", "near_each"), tok, 1
    )
    grad_bias = jnp.sum(received.astype(F32), axis=0)
    grad_activations = jnp.einsum("nt,fn->tf", grad_rows, proj_weight, preferred_element_type=F32).astype(BF16)
    grad_zg = jnp.einsum("jhi,ch->ijc", grad_bias, bias_weight, precision=lax.Precision.HIGHEST)
    weight_part = jnp.einsum("ijc,jhi->ch", scaled, grad_bias, precision=lax.Precision.HIGHEST)
    gain_part = jnp.sum(normed * grad_zg, axis=(0, 1))
    query_part = jnp.sum(grad_rows[:feature].astype(F32), axis=1)
    small = jnp.concatenate([query_part, weight_part.reshape(-1), gain_part])
    small = jnp.pad(small, (0, -small.size % 1024)).reshape(-1, 128)
    first = jnp.einsum("srt,snt->rn", act_near, rows_near, preferred_element_type=F32)
    second = jnp.einsum("srt,stn->rn", gated_near, cot_near, preferred_element_type=F32)
    terms = jnp.concatenate([first.astype(BF16), second.astype(BF16)], axis=1)
    terms, small = exchange((terms.reshape(outer, shard, -1), small), ("far_each", "all"), tok, 2)
    weight_grads = jnp.sum(terms.astype(F32), axis=0)
    small = jnp.sum(small, axis=0).reshape(-1)
    grad_norm = grad_zg * pair_gain
    grad_pair = (
        grad_norm
        - jnp.mean(grad_norm, axis=-1, keepdims=True)
        - normed * jnp.mean(grad_norm * normed, axis=-1, keepdims=True)
    ) * rstd
    split = feature + weight_part.size
    return (
        grad_activations.reshape(samples, tokens, feature),
        grad_pair.astype(BF16),
        weight_grads[:, : 4 * feature],
        weight_grads[:, 4 * feature :],
        small[:feature],
        small[feature:split].reshape(weight_part.shape),
        small[split : split + pair_gain.shape[0]],
    )


def solution(mesh):
    in_specs = (
        P(("groups", "tok"), None, None),
        P("groups", "tok", None),
        P(),
        P(),
        P(),
        P(),
        P(),
        P("groups"),
        P(("groups", "tok"), None, None),
    )
    out_specs = (
        P(("groups", "tok"), None, None),
        P("groups", "tok", None),
        P(("groups", "tok"), None),
        P(("groups", "tok"), None),
        P("groups"),
        P("groups", None),
        P("groups"),
    )
    return jax.shard_map(on_device, mesh=mesh, in_specs=in_specs, out_specs=out_specs, check_vma=False)
```
